32 devices in a mesh: seq: 8 (over z, x), head: 2 (over y), batch: 2 (over core).
Axes of the slice: x: 2, y: 2, z: 4, core: 2. Of those that a mesh axis runs over, the one named last changes fastest.
Arguments:
- queries: bfloat16 [2, 4096, 32, 128], P('batch', 'seq', 'head'), may hold values from -200 to 200
- key_states: bfloat16 [2, 4096, 8, 128], P('batch', 'seq', 'head'), may hold values from -7 to 7
- value_vectors: bfloat16 [2, 4096, 8, 128], P('batch', 'seq', 'head'), may hold values from -6 to 6
- block_doc: int32 [2, 32], P('batch'), may hold values from 0 to 7, never falling along the last dimension, each value on 1 to 20 neighbouring positions
- out_weight: bfloat16 [4096, 8192], P('head', 'batch'), may hold values from -0.5 to 0.5
Outputs:
- projected: bfloat16 [4096, 2, 8192], P(('seq', 'head'), None, 'batch')
The draws below stay inside these ranges and needn't reach their ends.
Inputs may be any that keep to these rules, and one draw needn't show every extreme that they name: block_doc[b, j] never falls along j, starts at 0 and skips no number; every document covers 1 to 20 whole blocks, and some document covers exactly 20.
All inputs are finite; a program needn't handle non-finite values.
Results may differ from the reference program's by a relative error of at most 0.0095.
Values may be sent and summed in bfloat16 or wider, within the bound.
A program may use at most 128 MiB of HBM per device.

```python
import math
import jax
import jax.numpy as jnp
import numpy as np
from jax import lax

D = 8192
QUERY_HEADS = 32
KEY_VALUE_HEADS = 8
HEAD_WIDTH = 128
BLK = 128
SEQUENCE_LENGTH = 4096
PACKED_BATCH = 2
NBLK = 32
MOSTB = 20
NDOC = 8
HQ_DEV = 16
HGROUPS = 2


def draw_pair(key):
    query_draw = jax.random.normal(jax.random.fold_in(key, 11), (PACKED_BATCH, SEQUENCE_LENGTH, QUERY_HEADS, HEAD_WIDTH), jnp.float32)
    key_sample = jnp.clip(jax.random.normal(jax.random.fold_in(key, 12), (PACKED_BATCH, SEQUENCE_LENGTH, KEY_VALUE_HEADS, HEAD_WIDTH), jnp.float32), -6.0, 6.0)
    query_draw = jnp.clip(query_draw, -6.0, 6.0)
    return (query_draw, key_sample)


def draw_queries(key, part):
    return draw_pair(key)[0].astype(jnp.bfloat16)


def draw_key_states(key, part):
    return draw_pair(key)[1].astype(jnp.bfloat16)


def shard_levels(stream_key, extent, cuts, low, top_value):
    loudness, own = 1.0, jax.random.fold_in(stream_key, 6)
    for dim, blocks in cuts:
        heights = jnp.exp(jax.random.uniform(jax.random.fold_in(own, dim), (blocks,), jnp.float32, low / len(cuts), top_value / len(cuts)))
        loudness = loudness * jnp.repeat(heights, extent[dim] // blocks).reshape([-1 if axis == dim else 1 for axis in range(len(extent))])
    return loudness


def profile(count, total, limit, slope):
    weights = [(1 << 20) // math.isqrt(grade ** slope) + 1 for grade in range(2, count + 1)]
    rest, given = total - limit - (count - 1), [1] * (count - 1)
    while rest > 0:
        free = [i for i in range(count - 1) if given[i] < limit]
        pool, budget = sum([weights[i] for i in free]), rest
        for i in free:
            addition = min(limit - given[i], max(1, budget * weights[i] // pool), rest)
            given[i] = given[i] + addition
            rest = rest - addition
    return np.array([limit] + given)


def ragged_sizes(key, amount, total, limit, lean):
    if amount == 2:
        one = jax.random.randint(key, (), max(1, total - limit), min(limit, total - 1) + 1)
        return jnp.stack([one, total - one])
    tallies = jnp.asarray(profile(amount, total, limit, lean), jnp.int32)
    pairs = (amount - 1) // 2
    source_of, receiver = tallies[1:1 + 2 * pairs:2], tallies[2:2 + 2 * pairs:2]
    slack = jnp.minimum(source_of - 1, limit - receiver)
    moved = jax.random.randint(jax.random.fold_in(key, 1), (pairs,), 0, 1 << 20) % (slack + 1)
    tallies = tallies.at[1:1 + 2 * pairs:2].set(source_of - moved).at[2:2 + 2 * pairs:2].set(receiver + moved)
    return tallies[jax.random.permutation(jax.random.fold_in(key, 2), amount)]


def gaussian(key, shape, spread, most, split=(), kind=jnp.bfloat16):
    drawn = spread * jax.random.normal(key, shape, jnp.float32)
    if split:
        drawn = drawn * shard_levels(key, shape, split, -0.22, 0.18)
    return jnp.clip(drawn, -most, most).astype(kind)


def setup_inputs(seed: int = 0) -> dict:
    streams_of = jax.random.split(jax.random.key(seed), 6)
    queries = draw_queries(jax.random.fold_in(streams_of[5], 71), 0)
    key_states = draw_key_states(jax.random.fold_in(streams_of[5], 71), 0)
    value_vectors = gaussian(streams_of[2], (PACKED_BATCH, SEQUENCE_LENGTH, KEY_VALUE_HEADS, HEAD_WIDTH), 1.0, 6.0, ((0, 2), (1, 8), (2, 2)))
    block_doc = jax.vmap(lambda own: jnp.searchsorted(jnp.cumsum(ragged_sizes(own, NDOC, NBLK, MOSTB, 2)), jnp.arange(NBLK), side="right"))(jax.random.split(streams_of[3], PACKED_BATCH)).reshape((PACKED_BATCH, NBLK)).astype(jnp.int32)
    out_weight = gaussian(streams_of[4], (QUERY_HEADS * HEAD_WIDTH, D), HEAD_WIDTH ** -0.5, 0.5, ((0, 2), (1, 2)))
    return {"queries": queries, "key_states": key_states, "value_vectors": value_vectors, "block_doc": block_doc, "out_weight": out_weight}


def reference(queries, key_states, value_vectors, block_doc, out_weight):
    group_count_per_key = QUERY_HEADS // KEY_VALUE_HEADS
    score_scale = HEAD_WIDTH ** -0.5
    positions = jnp.arange(SEQUENCE_LENGTH, dtype=jnp.int32)
    results = []
    for batch_index in range(PACKED_BATCH):
        doc_tok = jnp.repeat(block_doc[batch_index], BLK)
        visible = (doc_tok[:, None] == doc_tok[None, :]) & (positions[:, None] >= positions[None, :])
        query_seq = queries[batch_index]
        key_seq = key_states[batch_index]
        value_seq = value_vectors[batch_index]

        def head_out(head_index):
            q_head = lax.dynamic_index_in_dim(query_seq, head_index, 1, False)
            k_head = lax.dynamic_index_in_dim(key_seq, head_index // group_count_per_key, 1, False)
            v_head = lax.dynamic_index_in_dim(value_seq, head_index // group_count_per_key, 1, False)
            scores = jnp.dot(q_head, k_head.T, preferred_element_type=jnp.float32) * score_scale
            scores = jnp.where(visible, scores, -1e30)
            maxima = jnp.max(scores, axis=1)
            weights = jnp.where(visible, jnp.exp(scores - maxima[:, None]), 0.0)
            denominator = jnp.sum(weights, axis=1)
            numerator = jnp.dot(weights.astype(jnp.bfloat16), v_head, preferred_element_type=jnp.float32)
            return (numerator / denominator[:, None]).astype(jnp.bfloat16)

        attended = lax.map(head_out, jnp.arange(QUERY_HEADS, dtype=jnp.int32))
        flattened = jnp.transpose(attended, (1, 0, 2)).reshape(SEQUENCE_LENGTH, QUERY_HEADS * HEAD_WIDTH)
        group_width = HQ_DEV * HEAD_WIDTH
        summed = jnp.zeros((SEQUENCE_LENGTH, D), jnp.float32)
        for group_index in range(HGROUPS):
            lower = group_index * group_width
            partial_value = jnp.dot(flattened[:, lower:lower + group_width], out_weight[lower:lower + group_width], preferred_element_type=jnp.float32).astype(jnp.bfloat16)
            partial_value = lax.optimization_barrier(partial_value)
            summed = summed + partial_value.astype(jnp.float32)
        results.append(summed.astype(jnp.bfloat16))
    return jnp.stack(results, axis=1)
```

```python
import functools
import math

import jax
import jax.numpy as jnp
from jax import lax
from jax.experimental import pallas as pl
from jax.experimental.pallas import tpu as pltpu
from jax.sharding import PartitionSpec as P


HIDDEN = -1e30
MESH = pl.DeviceIdType.MESH


def move(array, axis, pairs):
    return lax.ppermute(array, axis, pairs)


def gather_plan(span):
    plan = [("own", 0)]
    for k in range(1, span // 2 + 1):
        plan.append(("same", k))
    for k in range(0, (span + 1) // 2 + 1):
        if 2 * k + 1 <= span or 1 <= 2 * k - 1 <= span:
            plan.append(("cross", k))
    return plan


def gather_shards(own, plan, span, seq_count):
    positions = range(seq_count)
    same = {0: own}
    result = []
    for kind, k in plan:
        if kind == "same":
            same[k] = move(same[k - 1], "seq", [(s, s + 2) for s in positions if s + 2 < seq_count])
    for kind, k in plan:
        if kind != "cross":
            result.append(same[k])
        elif k in same:
            pairs = []
            for s in positions:
                to = s + 1 if s % 2 == 0 else s - 1
                distance = to - s + 2 * k
                if 0 < distance <= span and to - distance >= 0 and to < seq_count:
                    pairs.append((s, to))
            result.append(move(same[k], "seq", pairs))
        else:
            pairs = [(s, s + 2 * k - 1) for s in positions if s % 2 == 1 and s + 2 * k - 1 < seq_count]
            result.append(move(own, "seq", pairs))
    return result


def gather_kernel(span, seq_count, ring_count, pieces, *refs):
    packs = refs[:ring_count]
    queries = refs[ring_count]
    own, out, q_out = refs[ring_count + 1 : ring_count + 4]
    swap_send, swap_recv, swap_copy, up_sems, cross_sems, far_sems, recv_sems = refs[ring_count + 4 :]
    me = lax.axis_index("seq")
    core = lax.axis_index("batch")
    even = lax.rem(me, 2) == 0
    odd = lax.rem(me, 2) == 1
    beside = me + 1 - 2 * lax.rem(me, 2)
    size = packs[0].shape[0] // pieces
    steps = span // 2
    far = span if span % 2 else 0
    q_wide = q_out.shape[2]

    barrier = pltpu.get_barrier_semaphore()
    friends = [(me + 2, me + 2 < seq_count), (me - 2, me >= 2), (beside, beside < seq_count)]
    if far:
        friends.append((me + far, odd & (me + far < seq_count)))
        friends.append((me - far, even & (me >= far)))
    peers = ring_count - 1

    def greet(friend):
        pl.semaphore_signal(barrier, inc=1, device_id={"seq": friend}, device_id_type=MESH)

    for friend, there in friends:
        pl.when(there)(functools.partial(greet, friend))
        peers = peers + there.astype(jnp.int32)
    for turn in range(1, ring_count):
        pl.semaphore_signal(
            barrier, inc=1, device_id={"batch": lax.rem(core + turn, ring_count)}, device_id_type=MESH
        )
    pl.semaphore_wait(barrier, peers)

    def swaps(n, kind):
        source = packs if kind == 0 else [queries.at[:, pl.ds(m * q_wide, q_wide)] for m in range(ring_count)]
        target = own.at[n] if kind == 0 else q_out.at[n]
        local = pltpu.make_async_copy(source[n], target, swap_copy.at[kind, n])
        away = [
            pltpu.make_async_remote_copy(
                src_ref=source[m],
                dst_ref=target,
                send_sem=swap_send.at[kind, m],
                recv_sem=swap_recv.at[kind, n],
                device_id={"batch": m},
                device_id_type=MESH,
            )
            for m in range(ring_count)
            if m != n
        ]
        return local, away

    def start_swaps(n, kind):
        local, away = swaps(n, kind)
        local.start()
        for copy in away:
            copy.start()

    def end_sends(n, kind):
        for copy in swaps(n, kind)[1]:
            copy.wait_send()

    def wait_swap(n, kind):
        local, away = swaps(n, kind)
        pl.when(core == n)(lambda: local.wait())
        pl.when(core != n)(lambda: away[0].wait_recv())

    for kind in (0, 1):
        for n in range(ring_count):
            pl.when(core == n)(functools.partial(start_swaps, n, kind))

    def part(ref, i):
        return ref.at[pl.ds(i * size, size)]

    def sending(source, i, slot, sem, to):
        return pltpu.make_async_remote_copy(
            src_ref=part(source, i),
            dst_ref=part(out.at[slot - 1], i),
            send_sem=sem,
            recv_sem=recv_sems.at[slot - 1, i],
            device_id={"seq": to},
            device_id_type=MESH,
        )

    def arrived(slot, i):
        sending(own.at[0], i, slot, recv_sems.at[slot - 1, i], me).wait_recv()

    def each_send(step, i, act):
        source = own.at[0] if step == 0 else out.at[2 * step - 1]
        there = me >= 2 * step
        if step < steps:
            pl.when(there & (me + 2 < seq_count))(
                lambda: act(sending(source, i, 2 * step + 2, up_sems.at[step, i], me + 2))
            )
        if 2 * step + 1 <= span:
            pl.when(there & even & (beside < seq_count))(
                lambda: act(sending(source, i, 2 * step + 1, cross_sems.at[step, i], beside))
            )
        if step > 0:
            pl.when(there & odd)(lambda: act(sending(source, i, 2 * step - 1, cross_sems.at[step, i], beside)))
        if step == 0 and far:
            pl.when(odd & (me + far < seq_count))(
                lambda: act(sending(source, i, far, far_sems.at[i], me + far))
            )

    wait_swap(0, 0)
    for i in range(pieces):
        each_send(0, i, lambda copy: copy.start())
    for step in range(1, steps + 1):
        for i in range(pieces):
            pl.when(me >= 2 * step)(functools.partial(arrived, 2 * step, i))
            each_send(step, i, lambda copy: copy.start())
    for n in range(ring_count):
        for kind in (0, 1):
            if n or kind:
                wait_swap(n, kind)
            pl.when(core == n)(functools.partial(end_sends, n, kind))
    for slot in range(1, span + 1, 2):
        for i in range(pieces):
            there = me >= slot
            if slot != far:
                there = there & (odd | (beside < seq_count))
            pl.when(there)(functools.partial(arrived, slot, i))
    for step in range(steps + 1):
        for i in range(pieces):
            each_send(step, i, lambda copy: copy.wait_send())


def gathered(packs, q_flat, span, seq_count):
    pieces = 4
    steps = span // 2
    count = len(packs)
    shape = packs[0].shape
    moved = span * packs[0].size * 2
    hbm = pl.BlockSpec(memory_space=pl.ANY)
    vmem = pl.BlockSpec(memory_space=pltpu.VMEM)
    dma = pltpu.SemaphoreType.DMA
    return pl.pallas_call(
        functools.partial(gather_kernel, span, seq_count, count, pieces),
        in_specs=[hbm] * (count + 1),
        out_specs=[vmem] * 3,
        out_shape=[
            jax.ShapeDtypeStruct((count, *shape), packs[0].dtype),
            jax.ShapeDtypeStruct((span, *shape), packs[0].dtype),
            jax.ShapeDtypeStruct((count, q_flat.shape[0], q_flat.shape[1] // count), q_flat.dtype),
        ],
        scratch_shapes=[
            dma((2, count)),
            dma((2, count)),
            dma((2, count)),
            dma((max(steps, 1), pieces)),
            dma((steps + 1, pieces)),
            dma((pieces,)),
            dma((span, pieces)),
        ],
        compiler_params=pltpu.CompilerParams(collective_id=0, has_side_effects=True),
        cost_estimate=pl.CostEstimate(flops=60 * 10**9, bytes_accessed=moved, transcendentals=0),
    )(*packs, q_flat)


def project_kernel(count, info, *refs):
    rows, weights, out_ref = refs[:count], refs[count : 2 * count], refs[2 * count]
    total = None
    for row, weight in zip(rows, weights):
        term = jnp.dot(row[...], weight[...], preferred_element_type=jnp.float32)
        total = term if total is None else total + term
    out_ref[...] = total.astype(out_ref.dtype)


def projected(info, rows, weight, begin, width):
    count = len(rows)
    height, deep = rows[0].shape
    step = min(512, width)

    def weight_spec(turn):
        return pl.BlockSpec((deep, step), lambda j, info: (info[turn], begin // step + j))

    return pl.pallas_call(
        functools.partial(project_kernel, count),
        grid_spec=pltpu.PrefetchScalarGridSpec(
            num_scalar_prefetch=1,
            grid=(width // step,),
            in_specs=[pl.BlockSpec((height, deep), lambda j, info: (0, 0))] * count
            + [weight_spec(turn) for turn in range(count)],
            out_specs=pl.BlockSpec((height, step), lambda j, info: (0, j)),
        ),
        out_shape=jax.ShapeDtypeStruct((height, width), rows[0].dtype),
        compiler_params=pltpu.CompilerParams(dimension_semantics=("arbitrary",)),
        cost_estimate=pl.CostEstimate(
            flops=2 * height * deep * count * width,
            bytes_accessed=2 * (height * deep * count + deep * count * width + height * width),
            transcendentals=0,
        ),
    )(info, *rows, *[weight] * count)


def attention_kernel(plan, span, block_len, group, head_dim, kv_heads, info, q_ref, *rest):
    count_in = len({where for _, _, where, _ in plan})
    arrays = rest[:count_in]
    out_ref, keys, values, score_a, score_b, accs, sems = rest[count_in:]
    shards = [arrays[where] if slot is None else arrays[where].at[slot] for _, _, where, slot in plan]
    wide = kv_heads * head_dim
    rows = keys.shape[0] // (span + 1)
    parts = rows // wide
    head = pl.program_id(0)
    tile = q_ref.shape[0]
    chunk = tile
    blocks = tile // block_len
    parity = info[0]
    diag = info[1]
    first_keys = [info[3 + b] for b in range(blocks)]

    @pl.when(head == 0)
    def _():
        def each(act):
            for i, (kind, k, _, _) in enumerate(plan):
                distance = {"cross": 2 * k - 1 + 2 * parity, "fixed": k}.get(kind, 2 * k)
                at = pl.multiple_of((span - distance) * rows, rows)

                def copies(i=i, at=at):
                    for part in range(parts):
                        source = shards[i].at[pl.ds(0, wide), pl.ds(part * wide, wide)]
                        act(pltpu.make_async_copy(source, keys.at[pl.ds(at + part * wide, wide)], sems.at[i, part]))
                    source = shards[i].at[pl.ds(wide, wide)]
                    act(pltpu.make_async_copy(source, values.at[:, pl.ds(at, rows)], sems.at[i, parts]))

                if kind == "cross":
                    pl.when((distance > 0) & (distance <= span))(copies)
                else:
                    copies()

        each(lambda copy: copy.start())
        each(lambda copy: copy.wait())

    lanes = pl.ds(pl.multiple_of(head * head_dim, head_dim), head_dim)
    factor = math.log2(math.e) / math.sqrt(head_dim)
    queries = [q_ref[:, a * head_dim : (a + 1) * head_dim].T for a in range(group)]

    def produce(t, target, first, masked, a):
        begin = pl.multiple_of(diag - t * chunk, chunk)
        s = jnp.dot(keys[pl.ds(begin, chunk), lanes], queries[a], preferred_element_type=jnp.float32)
        if masked:
            row = lax.broadcasted_iota(jnp.int32, (chunk, tile), 0)
            tok = lax.broadcasted_iota(jnp.int32, (chunk, tile), 1)
            edge = first_keys[0]
            for b in range(1, blocks):
                edge = jnp.where(tok < b * block_len, edge, first_keys[b])
            hide = row < edge - begin
            if first:
                hide = hide | (row > tok)
            s = jnp.where(hide, HIDDEN, s)
        target[:, a * tile : (a + 1) * tile] = s
        return jnp.max(s, axis=0, keepdims=True)

    def consume(t, source, state, a):
        top, fade, total = state
        begin = pl.multiple_of(diag - t * chunk, chunk)
        p = jnp.exp2((source[:, a * tile : (a + 1) * tile] - top) * factor)
        r = jnp.dot(values[lanes, pl.ds(begin, chunk)], p.astype(jnp.bfloat16), preferred_element_type=jnp.float32)
        accs[a] = accs[a] * fade + r
        return jnp.sum(p, axis=0, keepdims=True) + total * fade

    def joined(top, high, total):
        new = jnp.maximum(top, high)
        return new, jnp.exp2((top - new) * factor), total

    def full(t, now, later, state):
        done = []
        for a in range(group):
            high = produce(t + 1, later, False, False, a)
            total = consume(t, now, state[a], a)
            done.append(joined(state[a][0], high, total))
        return tuple(done)

    def pair(i, state):
        return full(2 * i + 1, score_b, score_a, full(2 * i, score_a, score_b, state))

    def single(t, state):
        done = []
        for a in range(group):
            total = consume(t, score_a, state[a], a)
            high = produce(t + 1, score_a, False, True, a)
            done.append(joined(state[a][0], high, total))
        return tuple(done)

    lowest = first_keys[0] // chunk
    clear = (first_keys[-1] + chunk - 1) // chunk
    last = diag // chunk
    count = last - lowest
    pairs = jnp.maximum(last - clear, 0) // 2
    state = []
    for a in range(group):
        top = produce(0, score_a, True, True, a)
        accs[a] = jnp.zeros((head_dim, tile), jnp.float32)
        state.append((top, jnp.ones((1, tile), jnp.float32), jnp.zeros((1, tile), jnp.float32)))
    state = lax.fori_loop(0, pairs, pair, tuple(state))
    state = lax.fori_loop(2 * pairs, count, single, state)
    for a in range(group):
        total = consume(count, score_a, state[a], a)
        out_ref[:, a * head_dim : (a + 1) * head_dim] = (accs[a] / total).T.astype(out_ref.dtype)


def attend(info, n, q_own, shards, plan, span, block_len, kv_heads, group, head_dim, tile):
    rows = shards[0].shape[-1]
    wide = group * head_dim
    work = 2 * 2 * tile * rows * 3 * kv_heads * group * head_dim
    return pl.pallas_call(
        functools.partial(attention_kernel, plan, span, block_len, group, head_dim, kv_heads),
        grid_spec=pltpu.PrefetchScalarGridSpec(
            num_scalar_prefetch=1,
            grid=(kv_heads,),
            in_specs=[pl.BlockSpec((None, tile, wide), lambda h, info: (n, info[2], h))]
            + [pl.BlockSpec(memory_space=pl.ANY)] * len(shards),
            out_specs=pl.BlockSpec((tile, wide), lambda h, info: (0, h)),
            scratch_shapes=[
                pltpu.VMEM(((span + 1) * rows, kv_heads * head_dim), jnp.bfloat16),
                pltpu.VMEM((kv_heads * head_dim, (span + 1) * rows), jnp.bfloat16),
                pltpu.VMEM((tile, group * tile), jnp.float32),
                pltpu.VMEM((tile, group * tile), jnp.float32),
                pltpu.VMEM((group, head_dim, tile), jnp.float32),
                pltpu.SemaphoreType.DMA((len(plan), rows // (kv_heads * head_dim) + 1)),
            ],
        ),
        out_shape=jax.ShapeDtypeStruct((tile, kv_heads * wide), jnp.bfloat16),
        compiler_params=pltpu.CompilerParams(dimension_semantics=("arbitrary",)),
        cost_estimate=pl.CostEstimate(
            flops=work, bytes_accessed=4 * (span + 1) * rows * kv_heads * head_dim, transcendentals=0
        ),
    )(info, q_own, *shards)


def on_device(queries, key_states, value_vectors, block_doc, out_weight):
    tok_rows, q_heads, head_dim = queries.shape[1:]
    kv_heads = key_states.shape[2]
    group = q_heads // kv_heads
    blocks_total = block_doc.shape[1]
    seq_count = lax.axis_size("seq")
    heads_count = lax.axis_size("head")
    batch_count = lax.axis_size("batch")
    block_len = tok_rows * seq_count // blocks_total
    seq_index = lax.axis_index("seq")
    head_index = lax.axis_index("head")
    batch_index = lax.axis_index("batch")
    blocks_dev = tok_rows // block_len
    longest = blocks_total // 2 + blocks_dev
    longest = longest + longest % 2
    span = (longest + blocks_dev - 2) // blocks_dev
    ring = range(batch_count)
    turns = range(1, batch_count)
    kv_part = kv_heads // batch_count
    wide = kv_part * head_dim
    part_rows = tok_rows // heads_count
    part_blocks = part_rows // block_len

    def chosen(pieces, index):
        picked = pieces[0]
        for n in range(1, batch_count):
            picked = jnp.where(index == n, pieces[n], picked)
        return picked

    def swapped(pieces):
        got = [chosen(pieces, batch_index)]
        for turn in turns:
            sent = chosen(pieces, lax.rem(batch_index + turn, batch_count))
            got.append(move(sent, "batch", [(i, (i + turn) % batch_count) for i in ring]))
        return [chosen([got[(c - n) % batch_count] for c in ring], batch_index) for n in ring]

    k_flat = key_states[0].reshape(tok_rows, kv_heads * head_dim)
    v_flat = value_vectors[0].reshape(tok_rows, kv_heads * head_dim).T
    packs = []
    for n in ring:
        mine = k_flat[:, n * wide : (n + 1) * wide]
        pieces = [mine[at : at + wide] for at in range(0, tok_rows, wide)]
        packs.append(jnp.concatenate([jnp.concatenate(pieces, axis=1), v_flat[n * wide : (n + 1) * wide]], axis=0))
    q_flat = queries[0].reshape(tok_rows, q_heads * head_dim)
    docs = swapped([block_doc[0]] * batch_count)

    hops = gather_plan(span)
    kv_own, fetched, q_own = gathered(packs, q_flat, span, seq_count)
    shards = [[kv_own, fetched]]
    plans = [[("fixed", 0, 0, 0)] + [("fixed", d, 1, d - 1) for d in range(1, span + 1)]]
    for n in range(1, batch_count):
        shards.append(gather_shards(kv_own[n], hops, span, seq_count))
        plans.append([(kind, k, i, None) for i, (kind, k) in enumerate(hops)])

    def info_of(n, tile):
        own_docs = lax.dynamic_slice_in_dim(docs[n], seq_index * blocks_dev + tile * part_blocks, part_blocks)
        first_block = jnp.sum((docs[n][None, :] < own_docs[:, None]).astype(jnp.int32), axis=1)
        first_key = (first_block - (seq_index - span) * blocks_dev) * block_len
        head = jnp.stack([seq_index % 2, span * tok_rows + tile * part_rows, tile]).astype(jnp.int32)
        return jnp.concatenate([head, first_key.astype(jnp.int32)])

    infos = {
        (n, hop): info_of(n, lax.rem(head_index + hop, heads_count)) for n in ring for hop in range(heads_count)
    }

    def after_of(value, after):
        if after is None:
            return value
        return lax.optimization_barrier((value, after))[0]

    def attended(n, hop, after):
        info = after_of(infos[n, hop], after)
        mine = attend(info, n, q_own, shards[n], plans[n], span, block_len, kv_part, group, head_dim, part_rows)
        got = [mine] + [
            move(mine, "batch", [(i, (i + turn) % batch_count) for i in ring]) for turn in turns
        ]
        return got

    owners = [lax.rem(batch_index - turn + batch_count, batch_count) for turn in ring]
    halves = jnp.stack(owners).astype(jnp.int32)
    columns = out_weight.shape[1]
    cut = columns // 2

    terms = [[] for _ in ring]
    kept = []
    after = None
    for n in ring:
        for hop in list(range(1, heads_count)) + [0]:
            got = attended(n, hop, after)
            if hop:
                sent = []
                for begin in range(0, columns, cut):
                    after = projected(after_of(halves, sent[-1] if sent else None), got, out_weight, begin, cut)
                    sent.append(after)
                for at, piece in enumerate(sent):
                    sent[at] = move(piece, "head", [(i, (i + hop) % heads_count) for i in range(heads_count)])
                terms[n].append(sent)
            else:
                kept.append(got)
                after = got[0]
    rows = [jnp.concatenate([got[turn] for got in kept], axis=0) for turn in ring]
    own = projected(after_of(halves, after), rows, out_weight, 0, columns)
    done = []
    for n in ring:
        total = own[n * part_rows : (n + 1) * part_rows].astype(jnp.float32)
        for sent in terms[n]:
            total = total + jnp.concatenate(sent, axis=1).astype(jnp.float32)
        done.append(total.astype(jnp.bfloat16))
    return jnp.stack(done, axis=1)


def solution(mesh):
    return jax.shard_map(
        on_device,
        mesh=mesh,
        in_specs=(
            P("batch", "seq", "head", None),
            P("batch", "seq", "head", None),
            P("batch", "seq", "head", None),
            P("batch", None),
            P("head", "batch"),
        ),
        out_specs=P(("seq", "head"), None, "batch"),
        check_vma=False,
    )
```
